32 devices in a mesh: groups: 2 (over y), assets: 8 (over z, x), tm: 2 (over core).
Axes of the slice: x: 2, y: 2, z: 4, core: 2. Of those that a mesh axis runs over, the one named last changes fastest.
Arguments:
- returns: bfloat16 [1536, 16384], P('tm', ('groups', 'assets')), parts along dimension 1, may hold values from -24 to 24
- prior: float32 [16384, 8192], P(('groups', 'assets')), parts along dimension 0, may hold values from -3 to 3
Outputs:
- covariance: float32 [2, 16384, 8192], P('tm', ('groups', 'assets')), parts along dimension 1
The draws below stay inside these ranges and needn't reach their ends.
There are 2 independent parts, one for each index of `groups`. The reference program is written for one: setup_inputs(seed, part) draws one part's arguments, and reference() takes and returns one part's arrays. A program takes and returns all parts, laid end to end along the dimension named above; each array names one. Nothing has to cross between parts.
All inputs are finite; a program needn't handle non-finite values.
Results may differ from the reference program's by a relative error of at most 0.0045.
Values may be sent and summed in bfloat16 or wider, within the bound.
A program may use at most 256 MiB of HBM per device.

```python
import jax
import jax.numpy as jnp
from jax import lax

ASSETS = 8192
MIN_DEV = 768
SLABS = 2
MINUTES = 1536


def block_levels(stream_key, dims, cuts, smallest, top_value):
    factor_of = 1.0
    for dim, blocks in cuts:
        steps = jax.random.uniform(jax.random.fold_in(jax.random.fold_in(stream_key, 6), dim), (blocks,), jnp.float32, smallest / len(cuts), top_value / len(cuts))
        factor_of = factor_of * jnp.repeat(jnp.exp(steps), dims[dim] // blocks).reshape((-1,) + (1,) * (len(dims) - 1 - dim))
    return factor_of


def scatter_about(stream_key, extent, width, reach, shards=(), held_as=jnp.bfloat16):
    drawn = jax.random.normal(stream_key, extent, jnp.float32) * width
    if len(shards) > 0:
        drawn = block_levels(stream_key, extent, shards, -0.22, 0.18) * drawn
    return jnp.clip(drawn, min=-reach, max=reach).astype(held_as)


def setup_inputs(seed: int = 0, part: int = 0) -> dict:
    streams_of = jax.random.split(jax.random.key(seed), 3)
    own_keys = jax.random.split(jax.random.fold_in(streams_of[2], part), 3)
    returns = scatter_about(own_keys[0], (MINUTES, ASSETS), 4.0, 24.0, ((0, 2), (1, 8)))
    prior = scatter_about(own_keys[1], (ASSETS, ASSETS), 0.5, 3.0, ((0, 8),), jnp.float32)
    return dict(returns=returns, prior=prior)


def reference(returns, prior):
    lam = jnp.float32(0.9995)
    position = jnp.arange(MIN_DEV, dtype=jnp.float32)
    weight = jnp.sqrt((jnp.float32(1.0) - lam) * jnp.power(lam, jnp.float32(MIN_DEV - 1) - position))
    factor = jnp.power(lam, jnp.float32(MIN_DEV))
    carry = prior
    results = []
    for slab in range(SLABS):
        piece = returns[slab * MIN_DEV:(slab + 1) * MIN_DEV]
        scaled = (piece.astype(jnp.float32) * weight[:, None]).astype(jnp.bfloat16).astype(jnp.float32)
        gram = jnp.dot(scaled.T, scaled, precision=lax.Precision.HIGHEST)
        carry = factor * carry + gram
        results.append(carry)
    return jnp.stack(results)
```

```python
import functools

import jax
import jax.numpy as jnp
from jax import lax
from jax.experimental import pallas as pl
from jax.experimental.pallas import tpu as pltpu
from jax.sharding import PartitionSpec as P


def weights_of(minutes):
    lam = jnp.float32(0.9995)
    position = jnp.arange(minutes, dtype=jnp.float32)
    weight = jnp.sqrt(
        (jnp.float32(1.0) - lam) * jnp.power(lam, jnp.float32(minutes - 1) - position)
    )
    return weight, jnp.power(lam, jnp.float32(minutes))


def scale(returns, weight):
    return (returns.astype(jnp.float32) * weight[:, None]).astype(jnp.bfloat16)


def local_general(returns, prior):
    minutes, _ = returns.shape
    weight, factor = weights_of(minutes)
    scaled = scale(returns, weight)
    tile = lax.dot_general(
        scaled,
        lax.all_gather(scaled, "assets", axis=1, tiled=True),
        (((0,), (0,)), ((), ())),
        preferred_element_type=jnp.float32,
    )
    mine = lax.axis_index("tm")
    everything = lax.all_gather(tile.astype(jnp.bfloat16), "tm")

    def turn(k, before):
        new = factor * before + everything[k].astype(jnp.float32)
        return jnp.where(k < mine, new, before)

    before = lax.fori_loop(0, lax.axis_size("tm"), turn, prior)
    return (factor * before + tile)[None]


def block_kernel(picks, places, coef, prior, lhs, lhs_early, *refs):
    out = refs[-1]
    later = places[1] == 1

    def emit(chunks):
        half = chunks[0].shape[1]
        for h in range(2):
            columns = slice(h * half, (h + 1) * half)
            mine, early = chunks[h], chunks[2 + h]

            @pl.when(later)
            def _():
                out[:, columns] = (
                    coef[0] * prior[:, columns]
                    + jnp.dot(lhs[...], mine[...], preferred_element_type=jnp.float32)
                    + coef[1]
                    * jnp.dot(lhs_early[...], early[...], preferred_element_type=jnp.float32)
                )

            @pl.when(jnp.logical_not(later))
            def _():
                out[:, columns] = coef[0] * prior[:, columns] + jnp.dot(
                    lhs[...], mine[...], preferred_element_type=jnp.float32
                )

    if picks == 1:
        emit(refs[:4])
    else:
        pl.when(places[2] == 0)(lambda: emit(refs[:4]))
        pl.when(places[2] == 1)(lambda: emit(refs[4:8]))


def write_block(held, places, coef, prior, lhs, lhs_early, choices):
    rows, total = prior.shape
    minutes, half = choices[0][0].shape
    width = 2 * half
    tile = rows // 4 if rows % 32 == 0 else rows
    chunks = [chunk for choice in choices for chunk in choice]
    window = pl.BlockSpec((tile, width), lambda i, places: (i, places[0]))
    side = pl.BlockSpec((tile, minutes), lambda i, places: (i, 0))
    whole = pl.BlockSpec((minutes, half), lambda i, places: (0, 0))
    specs = [pl.BlockSpec(memory_space=pltpu.SMEM), window, side, side]
    specs += [whole] * len(chunks)
    operands = [places, coef, prior, lhs, lhs_early, *chunks]
    aliases = {}
    if held is not None:
        specs.append(pl.BlockSpec(memory_space=pl.ANY))
        aliases = {len(operands): 0}
        operands.append(held)
    return pl.pallas_call(
        functools.partial(block_kernel, len(choices)),
        out_shape=jax.ShapeDtypeStruct((rows, total), jnp.float32),
        grid_spec=pltpu.PrefetchScalarGridSpec(
            num_scalar_prefetch=1, grid=(rows // tile,), in_specs=specs, out_specs=window
        ),
        input_output_aliases=aliases,
        compiler_params=pltpu.CompilerParams(vmem_limit_bytes=40 * 1024 * 1024),
        cost_estimate=pl.CostEstimate(
            flops=4 * rows * width * minutes,
            bytes_accessed=16 * rows * width,
            transcendentals=0,
        ),
    )(*operands)


def local_planned(returns, prior):
    minutes, width = returns.shape
    half = width // 2
    weight, factor = weights_of(minutes)
    count = lax.axis_size("assets")
    lines = count // 2
    me, slab = lax.axis_index("assets"), lax.axis_index("tm")
    row, column = me // 2, me % 2
    outer = jnp.logical_or(row == 0, row == lines - 1)
    last = lines - 1

    at = lambda r, c: r * 2 + c
    both = lambda pairs: [(a, b) for s, t in pairs for a, b in ((s, t), (t, s))]
    across = both([(at(r, 0), at(r, 1)) for r in range(lines)])
    across_outer = both([(at(r, 0), at(r, 1)) for r in (0, last)])
    inward = [(at(r, c), at(n, c)) for r, n in ((0, 1), (last, last - 1)) for c in (0, 1)]
    outward = [(b, a) for a, b in inward]
    centre = both([(at(1, c), at(last - 1, c)) for c in (0, 1)])
    send = lambda block, pairs: lax.ppermute(block, "assets", pairs)
    choose = lambda a, b: jnp.where(outer, a, b)

    own = [scale(returns[:, h * half : (h + 1) * half], weight) for h in (0, 1)]
    got = []
    for h in (0, 1):
        b = own[h]
        x0, o0, c0 = send(b, across), send(b, inward + outward), send(b, centre)
        x1 = send(choose(o0, c0), across)
        o1 = send(choose(x0, c0), inward + outward)
        c1 = send(o0, centre)
        x2 = send(choose(o1, c1), across)
        o2 = send(c1, outward)
        end = send(x2, outward) if h == 0 else send(o2, across_outer)
        got.append(dict(own=b, x0=x0, o0=o0, c0=c0, x1=x1, o1=o1, c1=c1, x2=x2, o2=o2, end=end))

    def chunks(name):
        mine = [got[h][name] for h in (0, 1)]
        return mine + [lax.ppermute(chunk, "tm", [(0, 1)]) for chunk in mine]

    names = ("own", "x0", "o0", "c0", "x1", "o1", "c1", "x2", "o2", "end")
    blocks = {name: chunks(name) for name in names}

    lhs = scale(returns, weight).T
    lhs_early = jnp.concatenate(blocks["own"][2:], axis=1).T
    later = (slab > 0).astype(jnp.int32)
    coef = jnp.stack([jnp.where(slab > 0, factor * factor, factor), factor])

    def place(distance_outer, other_outer, distance_inner, other_inner):
        distance = jnp.where(outer, distance_outer, distance_inner)
        line = jnp.where(row < lines // 2, distance, last - distance)
        other = jnp.where(outer, other_outer, other_inner)
        return line * 2 + jnp.where(other == 1, 1 - column, column)

    steps = (
        (("own",), (0, 0, 1, 0)),
        (("x0",), (0, 1, 1, 1)),
        (("o0",), (1, 0, 0, 0)),
        (("x1",), (1, 1, 2, 1)),
        (("o1",), (2, 0, 0, 1)),
        (("x2",), (2, 1, 3, 1)),
        (("o2", "c0"), (3, 0, 2, 0)),
        (("end", "c1"), (3, 1, 3, 0)),
    )
    held = None
    for picked, where in steps:
        places = jnp.stack(
            [place(*where), later, jnp.where(outer, 0, 1)]
        ).astype(jnp.int32)
        held = write_block(
            held, places, coef, prior, lhs, lhs_early, [blocks[name] for name in picked]
        )
    return held[None]


def solution(mesh):
    placed = (P("tm", ("groups", "assets")), P(("groups", "assets"), None))
    planned = mesh.shape["tm"] == 2 and mesh.shape["assets"] == 8

    def local(returns, prior):
        if planned and returns.shape[1] % 256 == 0 and returns.shape[0] % 16 == 0:
            return local_planned(returns, prior)
        return local_general(returns, prior)

    return jax.shard_map(
        local,
        mesh=mesh,
        in_specs=placed,
        out_specs=P("tm", ("groups", "assets"), None),
        check_vma=False,
    )
```
